32 devices in a mesh: grp: 2 (over y), row: 4 (over z), col: 2 (over x), cls: 2 (over core).
Axes of the slice: x: 2, y: 2, z: 4, core: 2. Of those that a mesh axis runs over, the one named last changes fastest.
Arguments:
- unary_scores: int32 [32, 16, 256], P('cls', ('grp', 'row'), 'col'), parts along dimension 1, may hold values from -256 to 256
- confidence: float32 [16, 256], P(('grp', 'row'), 'col'), parts along dimension 0, may hold values from 0.5 to 64
- features: bfloat16 [16, 256, 256], P(('grp', 'row'), 'col'), parts along dimension 0, may hold values from -12 to 12
- compat_table: int32 [32, 32], replicated, may hold values from 0 to 7
Outputs:
- belief: bfloat16 [32, 16, 256], P('cls', ('grp', 'row'), 'col'), parts along dimension 1
The draws below stay inside these ranges and needn't reach their ends.
There are 2 independent parts, one for each index of `grp`. The reference program is written for one: setup_inputs(seed, part) draws one part's arguments, and reference() takes and returns one part's arrays. A program takes and returns all parts, laid end to end along the dimension named above; an argument that names none is the same for every part. Nothing has to cross between parts.
All inputs are finite; a program needn't handle non-finite values.
Results may differ from the reference program's by a relative error of at most 0.0021.
Values may be sent and summed in bfloat16 or wider, within the bound.
A program may use at most 64 MiB of HBM per device.

```python
import math
import jax
import jax.numpy as jnp
from jax import lax

CLASSES = 32
LIVE = 21
R = 256
ROWS_DEV = 2
COLS_DEV = 128
H = 8
W = 256


def draw_confidence(key, part):
    key_base = jax.random.fold_in(key, 0)
    base = jnp.exp(jax.random.uniform(key_base, (H, W), jnp.float32, math.log(0.5), math.log(8.0)))
    return base


def draw_features(key, part):
    key_perm = jax.random.fold_in(key, 0)
    key_center = jax.random.fold_in(key, 1)
    key_noise = jax.random.fold_in(key, 2)
    key_mix = jax.random.fold_in(key, 4)
    key_roam = jax.random.fold_in(key, 5)
    col_blocks = W // COLS_DEV
    block_count = H // ROWS_DEV * col_blocks
    center_count = block_count // 2 + 1
    order = jax.random.permutation(key_perm, block_count)
    cluster = jnp.zeros((block_count,), jnp.int32).at[order].set(jnp.arange(block_count, dtype=jnp.int32) // 2)
    centers = jax.random.normal(key_center, (center_count, R), jnp.float32)
    block_of = (jnp.arange(H, dtype=jnp.int32) // ROWS_DEV)[:, None] * col_blocks + (jnp.arange(W, dtype=jnp.int32) // COLS_DEV)[None, :]
    stay_home = jax.random.randint(key_mix, (H, W), 0, 2, jnp.int32)
    roaming = jax.random.randint(key_roam, (H, W), 0, center_count, jnp.int32)
    pixel_cluster = jnp.where(stay_home == 1, cluster[block_of], roaming)
    base = centers[pixel_cluster]
    values = base + jax.random.normal(key_noise, (H, W, R), jnp.float32)
    return jnp.clip(values, -12.0, 12.0).astype(jnp.bfloat16)


def with_ends(drawn, stream_key, least, high):
    extent = drawn.shape
    spot = [jax.random.randint(jax.random.fold_in(stream_key, axis), (), 0, extent[axis]) for axis in range(len(extent))]
    drawn = drawn.at[tuple(spot)].set(least)
    longest = extent.index(max(extent))
    spot[longest] = (spot[longest] + 1) % extent[longest]
    return drawn.at[tuple(spot)].set(high)


def setup_inputs(seed: int = 0, part: int = 0) -> dict:
    arg_keys = jax.random.split(jax.random.key(seed), 5)
    part_splits = jax.random.split(jax.random.fold_in(arg_keys[4], part), 5)
    return {
        "unary_scores": with_ends(jax.random.randint(part_splits[0], (CLASSES, H, W), -256, 257), jax.random.fold_in(part_splits[0], 1), -256, 256).astype(jnp.int32),
        "confidence": draw_confidence(jax.random.fold_in(jax.random.fold_in(arg_keys[4], part), 71), part),
        "features": draw_features(jax.random.fold_in(jax.random.fold_in(arg_keys[4], part), 71), part),
        "compat_table": with_ends(jax.random.randint(arg_keys[3], (CLASSES, CLASSES), 0, 8), jax.random.fold_in(arg_keys[3], 1), 0, 7).astype(jnp.int32),
    }


unit_scale = 1.0 / 64.0
masked_low = -1.0e30


def class_softmax(logits, live_mask):
    class_top = jnp.max(jnp.where(live_mask, logits, masked_low), axis=0)
    raised = jnp.where(live_mask, jnp.exp(logits - class_top[None]), 0.0)
    return raised / jnp.sum(raised, axis=0)[None]


def reference(unary_scores, confidence, features, compat_table):
    classes, height, width = unary_scores.shape
    feat_depth = features.shape[2]
    pixels = height * width
    block_size = ROWS_DEV * COLS_DEV
    logits0 = confidence[None] * (unary_scores.astype(jnp.float32) * unit_scale)
    logits0 = logits0.reshape(classes, pixels)
    live_mask = (jnp.arange(classes, dtype=jnp.int32) < LIVE)[:, None]
    belief0 = class_softmax(logits0, live_mask).astype(jnp.bfloat16)
    flat_feats = features.reshape(pixels, feat_depth)
    feat_norm = jnp.sum(jnp.square(flat_feats.astype(jnp.float32)), axis=1)
    pixel_ids = jnp.arange(pixels, dtype=jnp.int32)

    def query_block(block_start):
        query_feats = lax.dynamic_slice_in_dim(flat_feats, block_start, block_size, 0)
        query_norm = lax.dynamic_slice_in_dim(feat_norm, block_start, block_size, 0)
        query_ids = block_start + jnp.arange(block_size, dtype=jnp.int32)
        scores = jnp.dot(query_feats, flat_feats.T, preferred_element_type=jnp.float32)
        spread = (query_norm[:, None] + feat_norm[None, :] - 2.0 * scores) * (2.0 / feat_depth)
        kernel = jnp.where(query_ids[:, None] == pixel_ids[None, :], 0.0, jnp.exp(4.0 - spread)).astype(jnp.bfloat16)
        summed = lax.dot_general(belief0, kernel, (((1,), (1,)), ((), ())), preferred_element_type=jnp.float32)
        return summed / (2.0 * block_size)

    starts = jnp.arange(pixels // block_size, dtype=jnp.int32) * block_size
    blocks = lax.map(query_block, starts)
    message = jnp.transpose(blocks, (1, 0, 2)).reshape(classes, pixels)
    potts_weight = compat_table.astype(jnp.float32) * (1.0 - jnp.eye(classes, dtype=jnp.float32))
    pairwise = jnp.dot(potts_weight, message, precision=lax.Precision.HIGHEST)
    logits1 = logits0 - pairwise
    belief = class_softmax(logits1, live_mask).astype(jnp.bfloat16)
    return belief.reshape(classes, height, width)
```

```python
import functools

import jax
import jax.numpy as jnp
from jax import lax
from jax.experimental import pallas as pl
from jax.experimental.pallas import tpu as pltpu
from jax.sharding import PartitionSpec as P

LIVE = 21

unit_scale = 1.0 / 64.0
masked_low = -1e30
MESH = pl.DeviceIdType.MESH
NT = (((1,), (1,)), ((), ()))


def class_softmax(logits, live_mask):
    class_top = jnp.max(jnp.where(live_mask, logits, masked_low), axis=0, keepdims=True)
    raised = jnp.where(live_mask, jnp.exp(logits - class_top), 0.0)
    return raised / jnp.sum(raised, axis=0, keepdims=True)


def spread_order(count):
    order = sorted(range(1, count), key=lambda o: (min(o, count - o), o))
    return order


def kernel(
    rows_n,
    cols_n,
    cls_n,
    unary_ref,
    conf_ref,
    feats_ref,
    compat_ref,
    out_ref,
    ubuf,
    kbuf,
    bbuf,
    qbuf,
    part,
    mbuf,
    fin,
    usend,
    urecv,
    ksend,
    krecv,
    bsend,
    brecv,
    qsend,
    qrecv,
    msend,
    mrecv,
):
    z = lax.axis_index("row")
    x = lax.axis_index("col")
    c = lax.axis_index("cls")
    share, row_count, col_count = unary_ref.shape
    depth = feats_ref.shape[2]
    classes = share * cls_n
    live_pad = mbuf.shape[-2]
    pixels = row_count * col_count
    half_rows = row_count // cls_n
    keys_local = half_rows * col_count

    def at_row(o):
        return {"row": lax.rem(z + o, rows_n)}

    def at_chip(xo, co):
        return {"col": lax.rem(x + xo, cols_n), "cls": lax.rem(c + co, cls_n)}

    returns = [(xo, co) for xo in range(cols_n) for co in range(cls_n) if xo or co]
    returns = sorted(returns, key=lambda p: (p[0] == 0, p))

    barrier = pltpu.get_barrier_semaphore()
    for o in range(1, rows_n):
        pl.semaphore_signal(barrier, inc=1, device_id=at_row(o), device_id_type=MESH)
    for xo, co in returns:
        pl.semaphore_signal(barrier, inc=1, device_id=at_chip(xo, co), device_id_type=MESH)
    pl.semaphore_wait(barrier, rows_n - 1 + len(returns))

    half = pl.ds(c * half_rows, half_rows)
    row_order = spread_order(rows_n)

    def row_copy(src, buf, o, ss, rs):
        return pltpu.make_async_remote_copy(
            src_ref=src,
            dst_ref=buf.at[o],
            send_sem=ss.at[o],
            recv_sem=rs.at[o],
            device_id=at_row(o),
            device_id_type=MESH,
        )

    ucopies = [
        pltpu.make_async_remote_copy(
            src_ref=unary_ref,
            dst_ref=ubuf.at[c],
            send_sem=usend.at[co],
            recv_sem=urecv.at[co],
            device_id=at_chip(0, co),
            device_id_type=MESH,
        )
        for co in range(1, cls_n)
    ]
    for copy in ucopies:
        copy.start()
    kcopies = {o: row_copy(feats_ref.at[half], kbuf, o, ksend, krecv) for o in row_order}
    for o in reversed(row_order):
        kcopies[o].start()
    qcopies = {
        xo: pltpu.make_async_remote_copy(
            src_ref=feats_ref,
            dst_ref=qbuf.at[xo],
            send_sem=qsend.at[xo],
            recv_sem=qrecv.at[xo],
            device_id=at_chip(xo, 0),
            device_id_type=MESH,
        )
        for xo in range(1, cols_n)
    }
    for xo in range(1, cols_n):
        qcopies[xo].start()

    ubuf[c] = unary_ref[...]
    live_mask = lax.broadcasted_iota(jnp.int32, (classes, 1), 0) < LIVE
    for copy in ucopies:
        copy.wait()

    def logits_of(r):
        conf = conf_ref[pl.ds(r, 1), :]
        scores = ubuf[:, :, pl.ds(r, 1), :].reshape(classes, col_count)
        return conf * (scores.astype(jnp.float32) * unit_scale)

    for r in range(half_rows):
        belief0 = class_softmax(logits_of(c * half_rows + r), live_mask)
        bbuf[0, :, r * col_count : (r + 1) * col_count] = belief0.astype(jnp.bfloat16)

    ones = jnp.ones((8, depth), jnp.bfloat16)
    scale = 2.0 / depth

    def query_of(xo):
        feats = feats_ref[...] if xo == 0 else qbuf[xo]
        feats = feats.reshape(pixels, depth)
        wide = feats.astype(jnp.float32)
        square = wide * wide
        high = square.astype(jnp.bfloat16)
        low = (square - high.astype(jnp.float32)).astype(jnp.bfloat16)
        norm = lax.dot_general(ones, high, NT, preferred_element_type=jnp.float32)
        norm = norm + lax.dot_general(ones, low, NT, preferred_element_type=jnp.float32)
        return feats, 2.0 - norm[:1] * scale

    def key_of(o):
        feats = feats_ref[half] if o == 0 else kbuf[o]
        feats = feats.reshape(keys_local, depth)
        wide = feats.astype(jnp.float32)
        return feats, 2.0 - jnp.sum(wide * wide, axis=1, keepdims=True) * scale

    def affinity(key, query, same):
        scores = lax.dot_general(key[0], query[0], NT, preferred_element_type=jnp.float32)
        value = jnp.exp(scores * (2.0 * scale) + (key[1] + query[1]))
        if same:
            place = c * keys_local + lax.broadcasted_iota(jnp.int32, (keys_local, pixels), 0)
            value = jnp.where(place == lax.broadcasted_iota(jnp.int32, (keys_local, pixels), 1), 0.0, value)
        return value.astype(jnp.bfloat16)

    def fold(belief, kern):
        return lax.dot_general(
            belief, kern, (((1,), (0,)), ((), ())), preferred_element_type=jnp.float32
        )

    own_query = query_of(0)
    own_key = key_of(0)
    first = affinity(own_key, own_query, True)

    bcopies = {o: row_copy(bbuf.at[0], bbuf, o, bsend, brecv) for o in row_order}
    for o in reversed(row_order):
        bcopies[o].start()

    own_belief = bbuf[0]
    sums = [fold(own_belief, first)]
    queries = [own_query]
    for xo in range(1, cols_n):
        qcopies[xo].wait_recv()
        queries.append(query_of(xo))
        sums.append(fold(own_belief, affinity(own_key, queries[xo], False)))
    for o in row_order:
        kcopies[o].wait_recv()
        key = key_of(o)
        kerns = [affinity(key, query, False) for query in queries]
        bcopies[o].wait_recv()
        belief = bbuf[o]
        sums = [total + fold(belief, kern) for total, kern in zip(sums, kerns)]

    for xo in range(cols_n):
        part[xo] = sums[xo][:live_pad]
    mcopies = {}
    for xo, co in returns:
        slot = xo * cls_n + co
        mcopies[slot] = pltpu.make_async_remote_copy(
            src_ref=part.at[xo],
            dst_ref=mbuf.at[slot],
            send_sem=msend.at[slot],
            recv_sem=mrecv.at[slot],
            device_id=at_chip(xo, co),
            device_id_type=MESH,
        )
        mcopies[slot].start()

    rows_i = lax.broadcasted_iota(jnp.int32, (live_pad, live_pad), 0)
    cols_i = lax.broadcasted_iota(jnp.int32, (live_pad, live_pad), 1)
    weight = jnp.where(rows_i == cols_i, 0.0, compat_ref[:live_pad, :live_pad].astype(jnp.float32))
    logits0 = jnp.concatenate([logits_of(r)[:live_pad] for r in range(row_count)], axis=1)
    message = sums[0][:live_pad]
    for slot in sorted(mcopies):
        mcopies[slot].wait_recv()
        message = message + mbuf[slot]
    message = message * (1.0 / (2.0 * pixels))
    pairwise = jnp.dot(
        weight, message, precision=lax.Precision.HIGHEST, preferred_element_type=jnp.float32
    )
    belief1 = class_softmax(logits0 - pairwise, live_mask[:live_pad])
    fin[:live_pad] = belief1
    if live_pad < classes:
        fin[live_pad:] = jnp.zeros((classes - live_pad, pixels), jnp.float32)
    out_ref[...] = fin[pl.ds(c * share, share), :].astype(jnp.bfloat16)

    for copies in (kcopies, bcopies, qcopies, mcopies):
        for copy in copies.values():
            copy.wait_send()


def body(unary_scores, confidence, features, compat_table):
    share, row_count, col_count = unary_scores.shape
    depth = features.shape[2]
    rows_n = lax.axis_size("row")
    cols_n = lax.axis_size("col")
    cls_n = lax.axis_size("cls")
    classes = share * cls_n
    live_pad = min(classes, -(-LIVE // 8) * 8)
    pixels = row_count * col_count
    half_rows = row_count // cls_n
    keys_local = half_rows * col_count
    dma = pltpu.SemaphoreType.DMA
    out = pl.pallas_call(
        functools.partial(kernel, rows_n, cols_n, cls_n),
        out_shape=jax.ShapeDtypeStruct((share, pixels), jnp.bfloat16),
        in_specs=[pl.BlockSpec(memory_space=pltpu.VMEM)] * 4,
        out_specs=pl.BlockSpec(memory_space=pltpu.VMEM),
        scratch_shapes=[
            pltpu.VMEM((cls_n, share, row_count, col_count), jnp.int32),
            pltpu.VMEM((rows_n, half_rows, col_count, depth), jnp.bfloat16),
            pltpu.VMEM((rows_n, classes, keys_local), jnp.bfloat16),
            pltpu.VMEM((cols_n, row_count, col_count, depth), jnp.bfloat16),
            pltpu.VMEM((cols_n, live_pad, pixels), jnp.float32),
            pltpu.VMEM((cols_n * cls_n, live_pad, pixels), jnp.float32),
            pltpu.VMEM((classes, pixels), jnp.float32),
            dma((cls_n,)),
            dma((cls_n,)),
            dma((rows_n,)),
            dma((rows_n,)),
            dma((rows_n,)),
            dma((rows_n,)),
            dma((cols_n,)),
            dma((cols_n,)),
            dma((cols_n * cls_n,)),
            dma((cols_n * cls_n,)),
        ],
        compiler_params=pltpu.CompilerParams(collective_id=0, has_side_effects=True),
    )(unary_scores, confidence, features, compat_table)
    return out.reshape(share, row_count, col_count)


def solution(mesh):
    in_specs = (
        P("cls", ("grp", "row"), "col"),
        P(("grp", "row"), "col"),
        P(("grp", "row"), "col", None),
        P(),
    )
    out_specs = P("cls", ("grp", "row"), "col")
    return jax.shard_map(body, mesh=mesh, in_specs=in_specs, out_specs=out_specs, check_vma=False)
```

```python
import functools

import jax
import jax.numpy as jnp
from jax import lax
from jax.experimental import pallas as pl
from jax.experimental.pallas import tpu as pltpu
from jax.sharding import PartitionSpec as P

LIVE = 21

unit_scale = 1.0 / 64.0
masked_low = -1e30
MESH = pl.DeviceIdType.MESH
NT = (((1,), (1,)), ((), ()))


def class_softmax(logits, live_mask):
    class_top = jnp.max(jnp.where(live_mask, logits, masked_low), axis=0, keepdims=True)
    raised = jnp.where(live_mask, jnp.exp(logits - class_top), 0.0)
    return raised / jnp.sum(raised, axis=0, keepdims=True)


def split_rows(rows_n):
    low = max(d for d in range(1, rows_n + 1) if rows_n % d == 0 and d * d <= rows_n)
    return low, rows_n // low


def kernel(
    low_n,
    high_n,
    cols_n,
    cls_n,
    unary_hbm,
    conf_hbm,
    feats_hbm,
    compat_hbm,
    out_ref,
    conf_ref,
    feats_ref,
    compat_ref,
    ubuf,
    kbuf,
    bbuf,
    qbuf,
    part,
    mbuf,
    fin,
    obuf,
    load,
    usend,
    urecv,
    ksend,
    krecv,
    fsend,
    frecv,
    bsend,
    brecv,
    qsend,
    qrecv,
    msend,
    mrecv,
    osend,
    orecv,
):
    z = lax.axis_index("row")
    x = lax.axis_index("col")
    c = lax.axis_index("cls")
    z_low = lax.rem(z, low_n)
    z_high = z // low_n
    _, share, row_count, col_count = ubuf.shape
    depth = feats_ref.shape[2]
    classes = share * cls_n
    live_pad = mbuf.shape[-2]
    pixels = row_count * col_count
    half_rows = row_count // cls_n
    keys_local = half_rows * col_count

    def at_query(slot):
        lo, xo = slot // cols_n, slot % cols_n
        row = z_high * low_n + lax.rem(z_low + lo, low_n)
        return {"row": row, "col": lax.rem(x + xo, cols_n)}

    def from_query(slot):
        lo, xo = slot // cols_n, slot % cols_n
        row = z_high * low_n + lax.rem(z_low + (low_n - lo), low_n)
        return {"row": row, "col": lax.rem(x + (cols_n - xo), cols_n)}

    def at_key(ho):
        return {"row": lax.rem(z_high + ho, high_n) * low_n + z_low}

    def at_core(co):
        return {"cls": lax.rem(c + co, cls_n)}

    query_slots = range(1, low_n * cols_n)
    key_slots = range(1, high_n)
    core_slots = range(1, cls_n)

    barrier = pltpu.get_barrier_semaphore()
    targets = [at_key(o) for o in key_slots]
    targets += [at_query(s) for s in query_slots]
    targets += [at_core(o) for o in core_slots]
    for target in targets:
        pl.semaphore_signal(barrier, inc=1, device_id=target, device_id_type=MESH)

    loads = [
        pltpu.make_async_copy(src, dst, load.at[i])
        for i, (src, dst) in enumerate(
            (
                (feats_hbm, feats_ref),
                (unary_hbm, ubuf.at[c]),
                (conf_hbm, conf_ref),
                (compat_hbm, compat_ref),
            )
        )
    ]
    for copy in loads:
        copy.start()
    for copy in loads:
        copy.wait()
    pl.semaphore_wait(barrier, len(targets))

    def remote(src, dst, ss, rs, target):
        return pltpu.make_async_remote_copy(
            src_ref=src,
            dst_ref=dst,
            send_sem=ss,
            recv_sem=rs,
            device_id=target,
            device_id_type=MESH,
        )

    half = pl.ds(c * half_rows, half_rows)
    kcopies = {
        o: remote(feats_ref.at[half], kbuf.at[o, c], ksend.at[o], krecv.at[o], at_key(o))
        for o in key_slots
    }
    ucopies = {
        o: remote(ubuf.at[c], ubuf.at[c], usend.at[o], urecv.at[o], at_core(o))
        for o in core_slots
    }
    qcopies = {
        s: remote(feats_ref.at[half], qbuf.at[s], qsend.at[s], qrecv.at[s], at_query(s))
        for s in query_slots
    }
    for o in key_slots:
        kcopies[o].start()
    for o in core_slots:
        ucopies[o].start()
    for s in reversed(query_slots):
        qcopies[s].start()

    ones = jnp.ones((8, depth), jnp.bfloat16)
    scale = 2.0 / depth

    def query_of(feats):
        feats = feats.reshape(keys_local, depth)
        wide = feats.astype(jnp.float32)
        square = wide * wide
        high = square.astype(jnp.bfloat16)
        low = (square - high.astype(jnp.float32)).astype(jnp.bfloat16)
        norm = lax.dot_general(ones, high, NT, preferred_element_type=jnp.float32)
        norm = norm + lax.dot_general(ones, low, NT, preferred_element_type=jnp.float32)
        return feats, 2.0 - norm[:1] * scale

    def key_of(feats):
        feats = feats.reshape(-1, depth)
        wide = feats.astype(jnp.float32)
        return feats, 2.0 - jnp.sum(wide * wide, axis=1, keepdims=True) * scale

    def affinity(key, query, same):
        scores = lax.dot_general(key[0], query[0], NT, preferred_element_type=jnp.float32)
        value = jnp.exp(scores * (2.0 * scale) + (key[1] + query[1]))
        if same:
            key_place = lax.broadcasted_iota(jnp.int32, value.shape, 0)
            query_place = c * keys_local + lax.broadcasted_iota(jnp.int32, value.shape, 1)
            value = jnp.where(key_place == query_place, 0.0, value)
        return value.astype(jnp.bfloat16)

    def fold(belief, kern):
        return lax.dot_general(
            belief, kern, (((1,), (0,)), ((), ())), preferred_element_type=jnp.float32
        )

    live_mask = lax.broadcasted_iota(jnp.int32, (classes, 1), 0) < LIVE
    for o in core_slots:
        ucopies[o].wait()

    def logits_of(r):
        conf = conf_ref[pl.ds(r, 1), :]
        scores = ubuf[:, :, pl.ds(r, 1), :].reshape(classes, col_count)
        return conf * (scores.astype(jnp.float32) * unit_scale)

    for r in range(row_count):
        belief0 = class_softmax(logits_of(r), live_mask).astype(jnp.bfloat16)
        h, start = r // half_rows, r % half_rows * col_count
        bbuf[0, h, :, start : start + col_count] = belief0

    own_key = key_of(feats_ref[...])
    queries = [query_of(feats_ref[half])]
    first = affinity(own_key, queries[0], True)

    bcopies = {
        o: remote(bbuf.at[0], bbuf.at[o], bsend.at[o], brecv.at[o], at_key(o)) for o in key_slots
    }
    for o in key_slots:
        bcopies[o].start()

    own_belief = jnp.concatenate([bbuf[0, h] for h in range(cls_n)], axis=1)
    sums = [fold(own_belief, first)]
    for s in query_slots:
        qcopies[s].wait_recv()
        queries.append(query_of(qbuf[s]))
        sums.append(fold(own_belief, affinity(own_key, queries[s], False)))

    fcopies = {}
    for o in key_slots:
        kcopies[o].wait_recv()
        for co in core_slots:
            fcopies[o, co] = remote(
                kbuf.at[o, c], kbuf.at[o, c], fsend.at[o, co], frecv.at[o, co], at_core(co)
            )
            fcopies[o, co].start()
    for o in key_slots:
        bcopies[o].wait_recv()
    for co in range(cls_n):
        source = lax.rem(c + (cls_n - co), cls_n)
        for o in key_slots:
            if co:
                fcopies[o, co].wait_recv()
            key = key_of(kbuf[o, source])
            belief = bbuf[o, source]
            sums = [
                total + fold(belief, affinity(key, query, False))
                for total, query in zip(sums, queries)
            ]

    for s in query_slots:
        part[s] = sums[s][:live_pad]
    mcopies = {
        s: remote(part.at[s], mbuf.at[s], msend.at[s], mrecv.at[s], from_query(s))
        for s in query_slots
    }
    for s in reversed(query_slots):
        mcopies[s].start()

    rows_i = lax.broadcasted_iota(jnp.int32, (live_pad, live_pad), 0)
    cols_i = lax.broadcasted_iota(jnp.int32, (live_pad, live_pad), 1)
    weight = jnp.where(rows_i == cols_i, 0.0, compat_ref[:live_pad, :live_pad].astype(jnp.float32))
    logits0 = jnp.concatenate(
        [logits_of(c * half_rows + r)[:live_pad] for r in range(half_rows)], axis=1
    )
    message = sums[0][:live_pad]
    for s in query_slots:
        mcopies[s].wait_recv()
        message = message + mbuf[s]
    message = message * (1.0 / (2.0 * pixels))
    pairwise = jnp.dot(
        weight, message, precision=lax.Precision.HIGHEST, preferred_element_type=jnp.float32
    )
    belief1 = class_softmax(logits0 - pairwise, live_mask[:live_pad])
    if live_pad < classes:
        belief1 = jnp.concatenate(
            [belief1, jnp.zeros((classes - live_pad, keys_local), jnp.float32)], axis=0
        )
    fin[...] = belief1.astype(jnp.bfloat16).reshape(cls_n, share, keys_local)
    ocopies = {
        o: remote(
            fin.at[lax.rem(c + o, cls_n)], obuf.at[c], osend.at[o], orecv.at[o], at_core(o)
        )
        for o in core_slots
    }
    for o in core_slots:
        ocopies[o].start()
    obuf[c] = fin[c]
    for o in core_slots:
        ocopies[o].wait_recv()
    out_ref[...] = jnp.concatenate([obuf[h] for h in range(cls_n)], axis=1)

    for copies in (kcopies, bcopies, qcopies, fcopies, mcopies, ocopies):
        for copy in copies.values():
            copy.wait_send()


def body(unary_scores, confidence, features, compat_table):
    share, row_count, col_count = unary_scores.shape
    depth = features.shape[2]
    low_n, high_n = split_rows(lax.axis_size("row"))
    cols_n = lax.axis_size("col")
    cls_n = lax.axis_size("cls")
    classes = share * cls_n
    live_pad = min(classes, -(-LIVE // 8) * 8)
    pixels = row_count * col_count
    half_rows = row_count // cls_n
    keys_local = half_rows * col_count
    query_n = low_n * cols_n
    bf16, f32 = jnp.bfloat16, jnp.float32
    dma = pltpu.SemaphoreType.DMA
    out = pl.pallas_call(
        functools.partial(kernel, low_n, high_n, cols_n, cls_n),
        out_shape=jax.ShapeDtypeStruct((share, pixels), bf16),
        in_specs=[pl.BlockSpec(memory_space=pl.ANY)] * 4,
        out_specs=pl.BlockSpec(memory_space=pltpu.VMEM),
        scratch_shapes=[
            pltpu.VMEM(confidence.shape, confidence.dtype),
            pltpu.VMEM(features.shape, features.dtype),
            pltpu.VMEM(compat_table.shape, compat_table.dtype),
            pltpu.VMEM((cls_n, share, row_count, col_count), jnp.int32),
            pltpu.VMEM((high_n, cls_n, half_rows, col_count, depth), bf16),
            pltpu.VMEM((high_n, cls_n, classes, keys_local), bf16),
            pltpu.VMEM((query_n, half_rows, col_count, depth), bf16),
            pltpu.VMEM((query_n, live_pad, keys_local), f32),
            pltpu.VMEM((query_n, live_pad, keys_local), f32),
            pltpu.VMEM((cls_n, share, keys_local), bf16),
            pltpu.VMEM((cls_n, share, keys_local), bf16),
            dma((4,)),
            dma((cls_n,)),
            dma((cls_n,)),
            dma((high_n,)),
            dma((high_n,)),
            dma((high_n, cls_n)),
            dma((high_n, cls_n)),
            dma((high_n,)),
            dma((high_n,)),
            dma((query_n,)),
            dma((query_n,)),
            dma((query_n,)),
            dma((query_n,)),
            dma((cls_n,)),
            dma((cls_n,)),
        ],
        compiler_params=pltpu.CompilerParams(collective_id=0, has_side_effects=True),
    )(unary_scores, confidence, features, compat_table)
    return out.reshape(share, row_count, col_count)


def solution(mesh):
    in_specs = (
        P("cls", ("grp", "row"), "col"),
        P(("grp", "row"), "col"),
        P(("grp", "row"), "col", None),
        P(),
    )
    out_specs = P("cls", ("grp", "row"), "col")
    return jax.shard_map(body, mesh=mesh, in_specs=in_specs, out_specs=out_specs, check_vma=False)
```

```python
import functools

import jax
import jax.numpy as jnp
from jax import lax
from jax.experimental import pallas as pl
from jax.experimental.pallas import tpu as pltpu
from jax.sharding import PartitionSpec as P

LIVE = 21

unit_scale = 1.0 / 64.0
masked_low = -1e30
MESH = pl.DeviceIdType.MESH
NT = (((1,), (1,)), ((), ()))


def class_softmax(logits, live_mask):
    class_top = jnp.max(jnp.where(live_mask, logits, masked_low), axis=0, keepdims=True)
    raised = jnp.where(live_mask, jnp.exp(logits - class_top), 0.0)
    return raised / jnp.sum(raised, axis=0, keepdims=True)


def split_rows(rows_n):
    low = max(d for d in range(1, rows_n + 1) if rows_n % d == 0 and d * d <= rows_n)
    return low, rows_n // low


def kernel(
    low_n,
    high_n,
    cols_n,
    cls_n,
    unary_hbm,
    conf_hbm,
    feats_hbm,
    compat_hbm,
    out_ref,
    conf_ref,
    feats_ref,
    compat_ref,
    ubuf,
    kbuf,
    bbuf,
    qbuf,
    part,
    mbuf,
    fin,
    obuf,
    load,
    usend,
    urecv,
    ksend,
    krecv,
    fsend,
    frecv,
    bsend,
    brecv,
    qsend,
    qrecv,
    msend,
    mrecv,
    osend,
    orecv,
):
    z = lax.axis_index("row")
    x = lax.axis_index("col")
    c = lax.axis_index("cls")
    z_low = lax.rem(z, low_n)
    z_high = z // low_n
    _, share, row_count, col_count = ubuf.shape
    depth = feats_ref.shape[2]
    classes = share * cls_n
    live_pad = mbuf.shape[-2]
    pixels = row_count * col_count
    half_rows = row_count // cls_n
    keys_local = half_rows * col_count

    def at_query(slot):
        lo, xo = slot // cols_n, slot % cols_n
        row = z_high * low_n + lax.rem(z_low + lo, low_n)
        return {"row": row, "col": lax.rem(x + xo, cols_n)}

    def from_query(slot):
        lo, xo = slot // cols_n, slot % cols_n
        row = z_high * low_n + lax.rem(z_low + (low_n - lo), low_n)
        return {"row": row, "col": lax.rem(x + (cols_n - xo), cols_n)}

    def at_key(ho):
        return {"row": lax.rem(z_high + ho, high_n) * low_n + z_low}

    def at_core(co):
        return {"cls": lax.rem(c + co, cls_n)}

    query_slots = range(1, low_n * cols_n)
    key_slots = range(1, high_n)
    core_slots = range(1, cls_n)

    barrier = pltpu.get_barrier_semaphore()
    targets = [at_key(o) for o in key_slots]
    targets += [at_query(s) for s in query_slots]
    targets += [at_core(o) for o in core_slots]
    for target in targets:
        pl.semaphore_signal(barrier, inc=1, device_id=target, device_id_type=MESH)

    loads = [
        pltpu.make_async_copy(src, dst, load.at[i])
        for i, (src, dst) in enumerate(
            (
                (feats_hbm, feats_ref),
                (unary_hbm, ubuf.at[c]),
                (conf_hbm, conf_ref),
                (compat_hbm, compat_ref),
            )
        )
    ]
    for copy in loads:
        copy.start()
    for copy in loads:
        copy.wait()
    pl.semaphore_wait(barrier, len(targets))

    def remote(src, dst, ss, rs, target):
        return pltpu.make_async_remote_copy(
            src_ref=src,
            dst_ref=dst,
            send_sem=ss,
            recv_sem=rs,
            device_id=target,
            device_id_type=MESH,
        )

    half = pl.ds(c * half_rows, half_rows)
    kcopies = {
        o: remote(feats_ref.at[half], kbuf.at[o, c], ksend.at[o], krecv.at[o], at_key(o))
        for o in key_slots
    }
    ucopies = {
        o: remote(ubuf.at[c], ubuf.at[c], usend.at[o], urecv.at[o], at_core(o))
        for o in core_slots
    }
    qcopies = {
        s: remote(feats_ref.at[half], qbuf.at[s], qsend.at[s], qrecv.at[s], at_query(s))
        for s in query_slots
    }
    for o in key_slots:
        kcopies[o].start()
    for o in core_slots:
        ucopies[o].start()
    near = [s for s in query_slots if s < cols_n]
    far = [s for s in query_slots if s >= cols_n]
    for s in near:
        qcopies[s].start()

    ones = jnp.ones((8, depth), jnp.bfloat16)
    scale = 2.0 / depth

    def query_of(feats):
        feats = feats.reshape(keys_local, depth)
        wide = feats.astype(jnp.float32)
        square = wide * wide
        high = square.astype(jnp.bfloat16)
        low = (square - high.astype(jnp.float32)).astype(jnp.bfloat16)
        norm = lax.dot_general(ones, high, NT, preferred_element_type=jnp.float32)
        norm = norm + lax.dot_general(ones, low, NT, preferred_element_type=jnp.float32)
        return feats, 2.0 - norm[:1] * scale

    def key_of(feats):
        feats = feats.reshape(-1, depth)
        wide = feats.astype(jnp.float32)
        return feats, 2.0 - jnp.sum(wide * wide, axis=1, keepdims=True) * scale

    def affinity(key, query, same):
        scores = lax.dot_general(key[0], query[0], NT, preferred_element_type=jnp.float32)
        value = jnp.exp(scores * (2.0 * scale) + (key[1] + query[1]))
        if same:
            key_place = lax.broadcasted_iota(jnp.int32, value.shape, 0)
            query_place = c * keys_local + lax.broadcasted_iota(jnp.int32, value.shape, 1)
            value = jnp.where(key_place == query_place, 0.0, value)
        return value.astype(jnp.bfloat16)

    def fold(belief, kern):
        return lax.dot_general(
            belief, kern, (((1,), (0,)), ((), ())), preferred_element_type=jnp.float32
        )

    live_mask = lax.broadcasted_iota(jnp.int32, (classes, 1), 0) < LIVE
    for o in core_slots:
        ucopies[o].wait()

    def logits_of(r):
        conf = conf_ref[pl.ds(r, 1), :]
        scores = ubuf[:, :, pl.ds(r, 1), :].reshape(classes, col_count)
        return conf * (scores.astype(jnp.float32) * unit_scale)

    for r in range(row_count):
        belief0 = class_softmax(logits_of(r), live_mask).astype(jnp.bfloat16)
        h, start = r // half_rows, r % half_rows * col_count
        bbuf[0, h, :, start : start + col_count] = belief0

    queries = [query_of(feats_ref[half])]

    bcopies = {
        o: remote(bbuf.at[0], bbuf.at[o], bsend.at[o], brecv.at[o], at_key(o)) for o in key_slots
    }
    for o in key_slots:
        bcopies[o].start()
    for s in reversed(far):
        qcopies[s].start()

    own_key = key_of(feats_ref[...])
    first = affinity(own_key, queries[0], True)
    own_belief = jnp.concatenate([bbuf[0, h] for h in range(cls_n)], axis=1)
    sums = [fold(own_belief, first)]
    for s in query_slots:
        qcopies[s].wait_recv()
        queries.append(query_of(qbuf[s]))
        sums.append(fold(own_belief, affinity(own_key, queries[s], False)))

    fcopies = {}
    for o in key_slots:
        kcopies[o].wait_recv()
        for co in core_slots:
            fcopies[o, co] = remote(
                kbuf.at[o, c], kbuf.at[o, c], fsend.at[o, co], frecv.at[o, co], at_core(co)
            )
            fcopies[o, co].start()
    for o in key_slots:
        bcopies[o].wait_recv()
    for co in range(cls_n):
        source = lax.rem(c + (cls_n - co), cls_n)
        for o in key_slots:
            if co:
                fcopies[o, co].wait_recv()
            key = key_of(kbuf[o, source])
            belief = bbuf[o, source]
            sums = [
                total + fold(belief, affinity(key, query, False))
                for total, query in zip(sums, queries)
            ]

    for s in query_slots:
        part[s] = sums[s][:live_pad]
    mcopies = {
        s: remote(part.at[s], mbuf.at[s], msend.at[s], mrecv.at[s], from_query(s))
        for s in query_slots
    }
    for s in reversed(query_slots):
        mcopies[s].start()

    rows_i = lax.broadcasted_iota(jnp.int32, (live_pad, live_pad), 0)
    cols_i = lax.broadcasted_iota(jnp.int32, (live_pad, live_pad), 1)
    weight = jnp.where(rows_i == cols_i, 0.0, compat_ref[:live_pad, :live_pad].astype(jnp.float32))
    logits0 = jnp.concatenate(
        [logits_of(c * half_rows + r)[:live_pad] for r in range(half_rows)], axis=1
    )
    message = sums[0][:live_pad]
    for s in query_slots:
        mcopies[s].wait_recv()
        message = message + mbuf[s]
    message = message * (1.0 / (2.0 * pixels))
    pairwise = jnp.dot(
        weight, message, precision=lax.Precision.HIGHEST, preferred_element_type=jnp.float32
    )
    belief1 = class_softmax(logits0 - pairwise, live_mask[:live_pad])
    if live_pad < classes:
        belief1 = jnp.concatenate(
            [belief1, jnp.zeros((classes - live_pad, keys_local), jnp.float32)], axis=0
        )
    fin[...] = belief1.astype(jnp.bfloat16).reshape(cls_n, share, keys_local)
    ocopies = {
        o: remote(
            fin.at[lax.rem(c + o, cls_n)], obuf.at[c], osend.at[o], orecv.at[o], at_core(o)
        )
        for o in core_slots
    }
    for o in core_slots:
        ocopies[o].start()
    obuf[c] = fin[c]
    for o in core_slots:
        ocopies[o].wait_recv()
    out_ref[...] = jnp.concatenate([obuf[h] for h in range(cls_n)], axis=1)

    for copies in (kcopies, bcopies, qcopies, fcopies, mcopies, ocopies):
        for copy in copies.values():
            copy.wait_send()


def body(unary_scores, confidence, features, compat_table):
    share, row_count, col_count = unary_scores.shape
    depth = features.shape[2]
    low_n, high_n = split_rows(lax.axis_size("row"))
    cols_n = lax.axis_size("col")
    cls_n = lax.axis_size("cls")
    classes = share * cls_n
    live_pad = min(classes, -(-LIVE // 8) * 8)
    pixels = row_count * col_count
    half_rows = row_count // cls_n
    keys_local = half_rows * col_count
    query_n = low_n * cols_n
    bf16, f32 = jnp.bfloat16, jnp.float32
    dma = pltpu.SemaphoreType.DMA
    out = pl.pallas_call(
        functools.partial(kernel, low_n, high_n, cols_n, cls_n),
        out_shape=jax.ShapeDtypeStruct((share, pixels), bf16),
        in_specs=[pl.BlockSpec(memory_space=pl.ANY)] * 4,
        out_specs=pl.BlockSpec(memory_space=pltpu.VMEM),
        scratch_shapes=[
            pltpu.VMEM(confidence.shape, confidence.dtype),
            pltpu.VMEM(features.shape, features.dtype),
            pltpu.VMEM(compat_table.shape, compat_table.dtype),
            pltpu.VMEM((cls_n, share, row_count, col_count), jnp.int32),
            pltpu.VMEM((high_n, cls_n, half_rows, col_count, depth), bf16),
            pltpu.VMEM((high_n, cls_n, classes, keys_local), bf16),
            pltpu.VMEM((query_n, half_rows, col_count, depth), bf16),
            pltpu.VMEM((query_n, live_pad, keys_local), f32),
            pltpu.VMEM((query_n, live_pad, keys_local), f32),
            pltpu.VMEM((cls_n, share, keys_local), bf16),
            pltpu.VMEM((cls_n, share, keys_local), bf16),
            dma((4,)),
            dma((cls_n,)),
            dma((cls_n,)),
            dma((high_n,)),
            dma((high_n,)),
            dma((high_n, cls_n)),
            dma((high_n, cls_n)),
            dma((high_n,)),
            dma((high_n,)),
            dma((query_n,)),
            dma((query_n,)),
            dma((query_n,)),
            dma((query_n,)),
            dma((cls_n,)),
            dma((cls_n,)),
        ],
        compiler_params=pltpu.CompilerParams(collective_id=0, has_side_effects=True),
    )(unary_scores, confidence, features, compat_table)
    return out.reshape(share, row_count, col_count)


def solution(mesh):
    in_specs = (
        P("cls", ("grp", "row"), "col"),
        P(("grp", "row"), "col"),
        P(("grp", "row"), "col", None),
        P(),
    )
    out_specs = P("cls", ("grp", "row"), "col")
    return jax.shard_map(body, mesh=mesh, in_specs=in_specs, out_specs=out_specs, check_vma=False)
```

```python
import functools

import jax
import jax.numpy as jnp
from jax import lax
from jax.experimental import pallas as pl
from jax.experimental.pallas import tpu as pltpu
from jax.sharding import PartitionSpec as P

LIVE = 21

unit_scale = 1.0 / 64.0
masked_low = -1e30
MESH = pl.DeviceIdType.MESH
NT = (((1,), (1,)), ((), ()))


def class_softmax(logits, live_mask):
    class_top = jnp.max(jnp.where(live_mask, logits, masked_low), axis=0, keepdims=True)
    raised = jnp.where(live_mask, jnp.exp(logits - class_top), 0.0)
    return raised / jnp.sum(raised, axis=0, keepdims=True)


def split_rows(rows_n):
    low = max(d for d in range(1, rows_n + 1) if rows_n % d == 0 and d * d <= rows_n)
    return low, rows_n // low


def kernel(
    low_n,
    high_n,
    cols_n,
    cls_n,
    unary_hbm,
    conf_hbm,
    feats_hbm,
    compat_hbm,
    out_ref,
    conf_ref,
    feats_ref,
    compat_ref,
    ubuf,
    kbuf,
    bbuf,
    qbuf,
    part,
    mbuf,
    fin,
    obuf,
    load,
    usend,
    urecv,
    ksend,
    krecv,
    fsend,
    frecv,
    bsend,
    brecv,
    qsend,
    qrecv,
    msend,
    mrecv,
    osend,
    orecv,
):
    z = lax.axis_index("row")
    x = lax.axis_index("col")
    c = lax.axis_index("cls")
    z_low = lax.rem(z, low_n)
    z_high = z // low_n
    _, share, row_count, col_count = ubuf.shape
    depth = feats_ref.shape[2]
    classes = share * cls_n
    live_pad = mbuf.shape[-2]
    pixels = row_count * col_count
    half_rows = row_count // cls_n
    keys_local = half_rows * col_count

    def at_query(slot):
        lo, xo = slot // cols_n, slot % cols_n
        row = z_high * low_n + lax.rem(z_low + lo, low_n)
        return {"row": row, "col": lax.rem(x + xo, cols_n)}

    def from_query(slot):
        lo, xo = slot // cols_n, slot % cols_n
        row = z_high * low_n + lax.rem(z_low + (low_n - lo), low_n)
        return {"row": row, "col": lax.rem(x + (cols_n - xo), cols_n)}

    def at_key(ho):
        return {"row": lax.rem(z_high + ho, high_n) * low_n + z_low}

    def at_core(co):
        return {"cls": lax.rem(c + co, cls_n)}

    query_slots = range(1, low_n * cols_n)
    key_slots = range(1, high_n)
    core_slots = range(1, cls_n)

    barrier = pltpu.get_barrier_semaphore()
    targets = [at_key(o) for o in key_slots]
    targets += [at_query(s) for s in query_slots]
    targets += [at_core(o) for o in core_slots]
    for target in targets:
        pl.semaphore_signal(barrier, inc=1, device_id=target, device_id_type=MESH)

    loads = [
        pltpu.make_async_copy(src, dst, load.at[i])
        for i, (src, dst) in enumerate(
            (
                (feats_hbm, feats_ref),
                (unary_hbm, ubuf.at[c]),
                (conf_hbm, conf_ref),
                (compat_hbm, compat_ref),
            )
        )
    ]
    for copy in loads:
        copy.start()
    for copy in loads:
        copy.wait()
    pl.semaphore_wait(barrier, len(targets))

    def remote(src, dst, ss, rs, target):
        return pltpu.make_async_remote_copy(
            src_ref=src,
            dst_ref=dst,
            send_sem=ss,
            recv_sem=rs,
            device_id=target,
            device_id_type=MESH,
        )

    half = pl.ds(c * half_rows, half_rows)
    kcopies = {
        o: remote(feats_ref.at[half], kbuf.at[o, c], ksend.at[o], krecv.at[o], at_key(o))
        for o in key_slots
    }
    ucopies = {
        o: remote(ubuf.at[c], ubuf.at[c], usend.at[o], urecv.at[o], at_core(o))
        for o in core_slots
    }
    qcopies = {
        s: remote(feats_ref.at[half], qbuf.at[s], qsend.at[s], qrecv.at[s], at_query(s))
        for s in query_slots
    }
    for o in key_slots:
        kcopies[o].start()
    for o in core_slots:
        ucopies[o].start()
    for s in reversed(query_slots):
        qcopies[s].start()

    ones = jnp.ones((8, depth), jnp.bfloat16)
    scale = 2.0 / depth

    def query_of(feats):
        feats = feats.reshape(-1, depth)
        wide = feats.astype(jnp.float32)
        square = wide * wide
        high = square.astype(jnp.bfloat16)
        low = (square - high.astype(jnp.float32)).astype(jnp.bfloat16)
        norm = lax.dot_general(ones, high, NT, preferred_element_type=jnp.float32)
        norm = norm + lax.dot_general(ones, low, NT, preferred_element_type=jnp.float32)
        return feats, 2.0 - norm[:1] * scale

    def key_of(feats):
        feats = feats.reshape(-1, depth)
        wide = feats.astype(jnp.float32)
        return feats, 2.0 - jnp.sum(wide * wide, axis=1, keepdims=True) * scale

    def affinity(key, query, same):
        scores = lax.dot_general(key[0], query[0], NT, preferred_element_type=jnp.float32)
        value = jnp.exp(scores * (2.0 * scale) + (key[1] + query[1]))
        if same:
            key_place = lax.broadcasted_iota(jnp.int32, value.shape, 0)
            lane = lax.broadcasted_iota(jnp.int32, value.shape, 1)
            mine = (lane < keys_local) & (key_place == c * keys_local + lane)
            value = jnp.where(mine, 0.0, value)
        return value.astype(jnp.bfloat16)

    def fold(belief, kern):
        return lax.dot_general(
            belief, kern, (((1,), (0,)), ((), ())), preferred_element_type=jnp.float32
        )

    live_mask = lax.broadcasted_iota(jnp.int32, (classes, 1), 0) < LIVE
    for o in core_slots:
        ucopies[o].wait()

    def logits_of(r):
        conf = conf_ref[pl.ds(r, 1), :]
        scores = ubuf[:, :, pl.ds(r, 1), :].reshape(classes, col_count)
        return conf * (scores.astype(jnp.float32) * unit_scale)

    for r in range(row_count):
        belief0 = class_softmax(logits_of(r), live_mask).astype(jnp.bfloat16)
        h, start = r // half_rows, r % half_rows * col_count
        bbuf[0, h, :, start : start + col_count] = belief0

    own_key = key_of(feats_ref[...])
    qbuf[0] = feats_ref[half]

    bcopies = {
        o: remote(bbuf.at[0], bbuf.at[o], bsend.at[o], brecv.at[o], at_key(o)) for o in key_slots
    }
    for o in key_slots:
        bcopies[o].start()

    own_belief = jnp.concatenate([bbuf[0, h] for h in range(cls_n)], axis=1)
    queries, sums = [], []

    def meet_group(lo):
        for s in range(max(1, lo * cols_n), (lo + 1) * cols_n):
            qcopies[s].wait_recv()
        queries.append(query_of(qbuf[lo * cols_n : (lo + 1) * cols_n]))
        sums.append(fold(own_belief, affinity(own_key, queries[lo], lo == 0)))

    meet_group(0)
    fcopies = {}
    for o in key_slots:
        kcopies[o].wait_recv()
        for co in core_slots:
            fcopies[o, co] = remote(
                kbuf.at[o, c], kbuf.at[o, c], fsend.at[o, co], frecv.at[o, co], at_core(co)
            )
            fcopies[o, co].start()
    for lo in range(1, low_n):
        meet_group(lo)
    keys, beliefs = [], []
    for o in key_slots:
        bcopies[o].wait_recv()
        for co in core_slots:
            fcopies[o, co].wait_recv()
        keys.append(key_of(kbuf[o]))
        beliefs.append(jnp.concatenate([bbuf[o, h] for h in range(cls_n)], axis=1))
    mcopies = {
        s: remote(part.at[s], mbuf.at[s], msend.at[s], mrecv.at[s], from_query(s))
        for s in query_slots
    }
    own_sum = None
    for lo in reversed(range(low_n)):
        total = sums[lo]
        for key, belief in zip(keys, beliefs):
            total = total + fold(belief, affinity(key, queries[lo], False))
        for xo in reversed(range(cols_n)):
            s = lo * cols_n + xo
            piece = total[:live_pad, xo * keys_local : (xo + 1) * keys_local]
            if s == 0:
                own_sum = piece
            else:
                part[s] = piece
                mcopies[s].start()

    rows_i = lax.broadcasted_iota(jnp.int32, (live_pad, live_pad), 0)
    cols_i = lax.broadcasted_iota(jnp.int32, (live_pad, live_pad), 1)
    weight = jnp.where(rows_i == cols_i, 0.0, compat_ref[:live_pad, :live_pad].astype(jnp.float32))
    logits0 = jnp.concatenate(
        [logits_of(c * half_rows + r)[:live_pad] for r in range(half_rows)], axis=1
    )
    message = own_sum
    for s in query_slots:
        mcopies[s].wait_recv()
        message = message + mbuf[s]
    message = message * (1.0 / (2.0 * pixels))
    pairwise = jnp.dot(
        weight, message, precision=lax.Precision.HIGHEST, preferred_element_type=jnp.float32
    )
    belief1 = class_softmax(logits0 - pairwise, live_mask[:live_pad])
    if live_pad < classes:
        belief1 = jnp.concatenate(
            [belief1, jnp.zeros((classes - live_pad, keys_local), jnp.float32)], axis=0
        )
    fin[...] = belief1.astype(jnp.bfloat16).reshape(cls_n, share, keys_local)
    ocopies = {
        o: remote(
            fin.at[lax.rem(c + o, cls_n)], obuf.at[c], osend.at[o], orecv.at[o], at_core(o)
        )
        for o in core_slots
    }
    for o in core_slots:
        ocopies[o].start()
    obuf[c] = fin[c]
    for o in core_slots:
        ocopies[o].wait_recv()
    out_ref[...] = jnp.concatenate([obuf[h] for h in range(cls_n)], axis=1)

    for copies in (kcopies, bcopies, qcopies, fcopies, mcopies, ocopies):
        for copy in copies.values():
            copy.wait_send()


def body(unary_scores, confidence, features, compat_table):
    share, row_count, col_count = unary_scores.shape
    depth = features.shape[2]
    low_n, high_n = split_rows(lax.axis_size("row"))
    cols_n = lax.axis_size("col")
    cls_n = lax.axis_size("cls")
    classes = share * cls_n
    live_pad = min(classes, -(-LIVE // 8) * 8)
    pixels = row_count * col_count
    half_rows = row_count // cls_n
    keys_local = half_rows * col_count
    query_n = low_n * cols_n
    bf16, f32 = jnp.bfloat16, jnp.float32
    dma = pltpu.SemaphoreType.DMA
    out = pl.pallas_call(
        functools.partial(kernel, low_n, high_n, cols_n, cls_n),
        out_shape=jax.ShapeDtypeStruct((share, pixels), bf16),
        in_specs=[pl.BlockSpec(memory_space=pl.ANY)] * 4,
        out_specs=pl.BlockSpec(memory_space=pltpu.VMEM),
        scratch_shapes=[
            pltpu.VMEM(confidence.shape, confidence.dtype),
            pltpu.VMEM(features.shape, features.dtype),
            pltpu.VMEM(compat_table.shape, compat_table.dtype),
            pltpu.VMEM((cls_n, share, row_count, col_count), jnp.int32),
            pltpu.VMEM((high_n, cls_n, half_rows, col_count, depth), bf16),
            pltpu.VMEM((high_n, cls_n, classes, keys_local), bf16),
            pltpu.VMEM((query_n, half_rows, col_count, depth), bf16),
            pltpu.VMEM((query_n, live_pad, keys_local), f32),
            pltpu.VMEM((query_n, live_pad, keys_local), f32),
            pltpu.VMEM((cls_n, share, keys_local), bf16),
            pltpu.VMEM((cls_n, share, keys_local), bf16),
            dma((4,)),
            dma((cls_n,)),
            dma((cls_n,)),
            dma((high_n,)),
            dma((high_n,)),
            dma((high_n, cls_n)),
            dma((high_n, cls_n)),
            dma((high_n,)),
            dma((high_n,)),
            dma((query_n,)),
            dma((query_n,)),
            dma((query_n,)),
            dma((query_n,)),
            dma((cls_n,)),
            dma((cls_n,)),
        ],
        compiler_params=pltpu.CompilerParams(collective_id=0, has_side_effects=True),
    )(unary_scores, confidence, features, compat_table)
    return out.reshape(share, row_count, col_count)


def solution(mesh):
    in_specs = (
        P("cls", ("grp", "row"), "col"),
        P(("grp", "row"), "col"),
        P(("grp", "row"), "col", None),
        P(),
    )
    out_specs = P("cls", ("grp", "row"), "col")
    return jax.shard_map(body, mesh=mesh, in_specs=in_specs, out_specs=out_specs, check_vma=False)
```

```python
import functools

import jax
import jax.numpy as jnp
from jax import lax
from jax.experimental import pallas as pl
from jax.experimental.pallas import tpu as pltpu
from jax.sharding import PartitionSpec as P

LIVE = 21

unit_scale = 1.0 / 64.0
masked_low = -1e30
MESH = pl.DeviceIdType.MESH
NT = (((1,), (1,)), ((), ()))


def class_softmax(logits, live_mask):
    class_top = jnp.max(jnp.where(live_mask, logits, masked_low), axis=0, keepdims=True)
    raised = jnp.where(live_mask, jnp.exp(logits - class_top), 0.0)
    return raised / jnp.sum(raised, axis=0, keepdims=True)


def split_rows(rows_n):
    low = max(d for d in range(1, rows_n + 1) if rows_n % d == 0 and d * d <= rows_n)
    return low, rows_n // low


def kernel(
    low_n,
    high_n,
    cols_n,
    cls_n,
    unary_hbm,
    conf_hbm,
    feats_hbm,
    compat_hbm,
    out_ref,
    conf_ref,
    feats_ref,
    compat_ref,
    ubuf,
    kbuf,
    bbuf,
    qbuf,
    part,
    mbuf,
    fin,
    obuf,
    load,
    usend,
    urecv,
    ksend,
    krecv,
    fsend,
    frecv,
    bsend,
    brecv,
    qsend,
    qrecv,
    msend,
    mrecv,
    osend,
    orecv,
):
    z = lax.axis_index("row")
    x = lax.axis_index("col")
    c = lax.axis_index("cls")
    z_low = lax.rem(z, low_n)
    z_high = z // low_n
    _, share, row_count, col_count = ubuf.shape
    depth = feats_ref.shape[2]
    classes = share * cls_n
    live_pad = mbuf.shape[-2]
    pixels = row_count * col_count
    half_rows = row_count // cls_n
    keys_local = half_rows * col_count

    def at_query(slot):
        lo, xo = slot // cols_n, slot % cols_n
        row = z_high * low_n + lax.rem(z_low + lo, low_n)
        return {"row": row, "col": lax.rem(x + xo, cols_n)}

    def from_query(slot):
        lo, xo = slot // cols_n, slot % cols_n
        row = z_high * low_n + lax.rem(z_low + (low_n - lo), low_n)
        return {"row": row, "col": lax.rem(x + (cols_n - xo), cols_n)}

    def at_key(ho):
        return {"row": lax.rem(z_high + ho, high_n) * low_n + z_low}

    def at_core(co):
        return {"cls": lax.rem(c + co, cls_n)}

    query_slots = range(1, low_n * cols_n)
    key_slots = range(1, high_n)
    core_slots = range(1, cls_n)

    barrier = pltpu.get_barrier_semaphore()
    targets = [at_key(o) for o in key_slots]
    targets += [at_query(s) for s in query_slots]
    targets += [at_core(o) for o in core_slots]
    for target in targets:
        pl.semaphore_signal(barrier, inc=1, device_id=target, device_id_type=MESH)

    loads = [
        pltpu.make_async_copy(src, dst, load.at[i])
        for i, (src, dst) in enumerate(
            (
                (feats_hbm, feats_ref),
                (unary_hbm, ubuf.at[c]),
                (conf_hbm, conf_ref),
                (compat_hbm, compat_ref),
            )
        )
    ]
    for copy in loads:
        copy.start()
    for copy in loads:
        copy.wait()
    pl.semaphore_wait(barrier, len(targets))

    def remote(src, dst, ss, rs, target):
        return pltpu.make_async_remote_copy(
            src_ref=src,
            dst_ref=dst,
            send_sem=ss,
            recv_sem=rs,
            device_id=target,
            device_id_type=MESH,
        )

    half = pl.ds(c * half_rows, half_rows)
    kcopies = {
        o: remote(feats_ref.at[half], kbuf.at[o, c], ksend.at[o], krecv.at[o], at_key(o))
        for o in key_slots
    }
    ucopies = {
        o: remote(ubuf.at[c], ubuf.at[c], usend.at[o], urecv.at[o], at_core(o))
        for o in core_slots
    }
    qcopies = {
        s: remote(feats_ref.at[half], qbuf.at[s], qsend.at[s], qrecv.at[s], at_query(s))
        for s in query_slots
    }
    for o in key_slots:
        kcopies[o].start()
    for o in core_slots:
        ucopies[o].start()
    for s in reversed(query_slots):
        qcopies[s].start()

    ones = jnp.ones((8, depth), jnp.bfloat16)
    scale = 2.0 / depth

    def query_of(feats):
        feats = feats.reshape(-1, depth)
        wide = feats.astype(jnp.float32)
        square = wide * wide
        high = square.astype(jnp.bfloat16)
        low = (square - high.astype(jnp.float32)).astype(jnp.bfloat16)
        norm = lax.dot_general(ones, high, NT, preferred_element_type=jnp.float32)
        norm = norm + lax.dot_general(ones, low, NT, preferred_element_type=jnp.float32)
        return feats, 2.0 - norm[:1] * scale

    def key_of(feats):
        feats = feats.reshape(-1, depth)
        wide = feats.astype(jnp.float32)
        return feats, 2.0 - jnp.sum(wide * wide, axis=1, keepdims=True) * scale

    def affinity(key, query, same):
        scores = lax.dot_general(key[0], query[0], NT, preferred_element_type=jnp.float32)
        value = jnp.exp(scores * (2.0 * scale) + (key[1] + query[1]))
        if same:
            key_place = lax.broadcasted_iota(jnp.int32, value.shape, 0)
            lane = lax.broadcasted_iota(jnp.int32, value.shape, 1)
            mine = (lane < keys_local) & (key_place == c * keys_local + lane)
            value = jnp.where(mine, 0.0, value)
        return value.astype(jnp.bfloat16)

    def fold(belief, kern):
        return lax.dot_general(
            belief, kern, (((1,), (0,)), ((), ())), preferred_element_type=jnp.float32
        )

    live_mask = lax.broadcasted_iota(jnp.int32, (classes, 1), 0) < LIVE
    for o in core_slots:
        ucopies[o].wait()

    def logits_of(r):
        conf = conf_ref[pl.ds(r, 1), :]
        scores = ubuf[:, :, pl.ds(r, 1), :].reshape(classes, col_count)
        return conf * (scores.astype(jnp.float32) * unit_scale)

    for r in range(row_count):
        belief0 = class_softmax(logits_of(r), live_mask).astype(jnp.bfloat16)
        h, start = r // half_rows, r % half_rows * col_count
        bbuf[0, h, :, start : start + col_count] = belief0

    own_key = key_of(feats_ref[...])
    qbuf[0] = feats_ref[half]

    bcopies = {
        o: remote(bbuf.at[0], bbuf.at[o], bsend.at[o], brecv.at[o], at_key(o)) for o in key_slots
    }
    for o in key_slots:
        bcopies[o].start()

    own_belief = jnp.concatenate([bbuf[0, h] for h in range(cls_n)], axis=1)
    queries, sums = [], []

    def meet_group(lo):
        for s in range(max(1, lo * cols_n), (lo + 1) * cols_n):
            qcopies[s].wait_recv()
        queries.append(query_of(qbuf[lo * cols_n : (lo + 1) * cols_n]))
        sums.append(fold(own_belief, affinity(own_key, queries[lo], lo == 0)))

    meet_group(0)
    fcopies = {}
    for o in key_slots:
        kcopies[o].wait_recv()
        for co in core_slots:
            fcopies[o, co] = remote(
                kbuf.at[o, c], kbuf.at[o, c], fsend.at[o, co], frecv.at[o, co], at_core(co)
            )
            fcopies[o, co].start()
    for lo in range(1, low_n):
        meet_group(lo)
    keys, beliefs = [], []
    for o in key_slots:
        bcopies[o].wait_recv()
        for co in core_slots:
            fcopies[o, co].wait_recv()
        keys.append(key_of(kbuf[o]))
        beliefs.append(jnp.concatenate([bbuf[o, h] for h in range(cls_n)], axis=1))
    mcopies = {
        s: remote(part.at[s], mbuf.at[s], msend.at[s], mrecv.at[s], from_query(s))
        for s in query_slots
    }
    own_sum = None
    for lo in reversed(range(low_n)):
        total = sums[lo]
        for key, belief in zip(keys, beliefs):
            total = total + fold(belief, affinity(key, queries[lo], False))
        for xo in reversed(range(cols_n)):
            s = lo * cols_n + xo
            piece = total[:live_pad, xo * keys_local : (xo + 1) * keys_local]
            if s == 0:
                own_sum = piece
            else:
                part[s] = piece
                mcopies[s].start()

    rows_i = lax.broadcasted_iota(jnp.int32, (live_pad, live_pad), 0)
    cols_i = lax.broadcasted_iota(jnp.int32, (live_pad, live_pad), 1)
    weight = jnp.where(rows_i == cols_i, 0.0, compat_ref[:live_pad, :live_pad].astype(jnp.float32))
    logits0 = jnp.concatenate(
        [logits_of(c * half_rows + r)[:live_pad] for r in range(half_rows)], axis=1
    )
    message = own_sum
    for s in query_slots:
        mcopies[s].wait_recv()
        message = message + mbuf[s]
    message = message * (1.0 / (2.0 * pixels))
    high = message.astype(jnp.bfloat16)
    rest = message - high.astype(jnp.float32)
    middle = rest.astype(jnp.bfloat16)
    low = (rest - middle.astype(jnp.float32)).astype(jnp.bfloat16)
    pieces = jnp.concatenate([high, middle, low], axis=0)
    pairwise = fold(jnp.concatenate([weight.astype(jnp.bfloat16)] * 3, axis=1), pieces)
    belief1 = class_softmax(logits0 - pairwise, live_mask[:live_pad])
    if live_pad < classes:
        belief1 = jnp.concatenate(
            [belief1, jnp.zeros((classes - live_pad, keys_local), jnp.float32)], axis=0
        )
    fin[...] = belief1.astype(jnp.bfloat16).reshape(cls_n, share, keys_local)
    ocopies = {
        o: remote(
            fin.at[lax.rem(c + o, cls_n)], obuf.at[c], osend.at[o], orecv.at[o], at_core(o)
        )
        for o in core_slots
    }
    for o in core_slots:
        ocopies[o].start()
    obuf[c] = fin[c]
    for o in core_slots:
        ocopies[o].wait_recv()
    out_ref[...] = jnp.concatenate([obuf[h] for h in range(cls_n)], axis=1)

    for copies in (kcopies, bcopies, qcopies, fcopies, mcopies, ocopies):
        for copy in copies.values():
            copy.wait_send()


def body(unary_scores, confidence, features, compat_table):
    share, row_count, col_count = unary_scores.shape
    depth = features.shape[2]
    low_n, high_n = split_rows(lax.axis_size("row"))
    cols_n = lax.axis_size("col")
    cls_n = lax.axis_size("cls")
    classes = share * cls_n
    live_pad = min(classes, -(-LIVE // 8) * 8)
    pixels = row_count * col_count
    half_rows = row_count // cls_n
    keys_local = half_rows * col_count
    query_n = low_n * cols_n
    bf16, f32 = jnp.bfloat16, jnp.float32
    dma = pltpu.SemaphoreType.DMA
    out = pl.pallas_call(
        functools.partial(kernel, low_n, high_n, cols_n, cls_n),
        out_shape=jax.ShapeDtypeStruct((share, pixels), bf16),
        in_specs=[pl.BlockSpec(memory_space=pl.ANY)] * 4,
        out_specs=pl.BlockSpec(memory_space=pltpu.VMEM),
        scratch_shapes=[
            pltpu.VMEM(confidence.shape, confidence.dtype),
            pltpu.VMEM(features.shape, features.dtype),
            pltpu.VMEM(compat_table.shape, compat_table.dtype),
            pltpu.VMEM((cls_n, share, row_count, col_count), jnp.int32),
            pltpu.VMEM((high_n, cls_n, half_rows, col_count, depth), bf16),
            pltpu.VMEM((high_n, cls_n, classes, keys_local), bf16),
            pltpu.VMEM((query_n, half_rows, col_count, depth), bf16),
            pltpu.VMEM((query_n, live_pad, keys_local), f32),
            pltpu.VMEM((query_n, live_pad, keys_local), f32),
            pltpu.VMEM((cls_n, share, keys_local), bf16),
            pltpu.VMEM((cls_n, share, keys_local), bf16),
            dma((4,)),
            dma((cls_n,)),
            dma((cls_n,)),
            dma((high_n,)),
            dma((high_n,)),
            dma((high_n, cls_n)),
            dma((high_n, cls_n)),
            dma((high_n,)),
            dma((high_n,)),
            dma((query_n,)),
            dma((query_n,)),
            dma((query_n,)),
            dma((query_n,)),
            dma((cls_n,)),
            dma((cls_n,)),
        ],
        compiler_params=pltpu.CompilerParams(collective_id=0, has_side_effects=True),
    )(unary_scores, confidence, features, compat_table)
    return out.reshape(share, row_count, col_count)


def solution(mesh):
    in_specs = (
        P("cls", ("grp", "row"), "col"),
        P(("grp", "row"), "col"),
        P(("grp", "row"), "col", None),
        P(),
    )
    out_specs = P("cls", ("grp", "row"), "col")
    return jax.shard_map(body, mesh=mesh, in_specs=in_specs, out_specs=out_specs, check_vma=False)
```
